32 devices in a mesh: band: 2 (over x), tm: 16 (over z, y, core).
Axes of the slice: x: 2, y: 2, z: 4, core: 2. Of those that a mesh axis runs over, the one named last changes fastest.
Arguments:
- volts: int32 [8, 2, 3145728], P('band', None, 'tm'), parts along dimension 0, may hold values from -128 to 127, as said below
- taps: float32 [16, 4096], replicated, may hold values from -0.024 to 0.024
- pairs: int32 [4, 2], replicated, may hold values from 0 to 3, as said below
Outputs:
- coherence: float32 [8, 4096], P('band'), parts along dimension 0
- normalized: float32 [2, 8, 768, 4096], P(None, 'band', 'tm'), parts along dimension 1
The draws below stay inside these ranges and needn't reach their ends.
There are 2 independent parts, one for each index of `band`. The reference program is written for one: setup_inputs(seed, part) draws one part's arguments, and reference() takes and returns one part's arrays. A program takes and returns all parts, laid end to end along the dimension named above; an argument that names none is the same for every part. Nothing has to cross between parts.
Inputs may be any that keep to these rules, and one draw needn't show every extreme that they name: `volts`: every sample is a whole number of the int8 range. Each pair names a stream of the first antenna (0 or 1) and then one of the second antenna (2 or 3); the four pairs are distinct.
All inputs are finite; a program needn't handle non-finite values.
Results may differ from the reference program's by a relative error of at most 0.000067.
Values sent between devices are 32-bit elements; how exact they have to be, the bound alone decides.
A program may use at most 128 MiB of HBM per device.

```python
import jax
import jax.numpy as jnp
from jax import lax

STREAMS = 4
TAPS = 16
CHANNELS = 4096
FRAMES = 768
SAMPLES = 3145728


def draw_volts(key, part):
    common_key = jax.random.fold_in(key, 11)
    noise_key = jax.random.fold_in(key, 12)
    weight_key = jax.random.fold_in(key, 13)
    delay_key = jax.random.fold_in(key, 14)
    common = jax.random.randint(common_key, (2, SAMPLES), -64, 64)
    noise = jax.random.randint(noise_key, (STREAMS, 2, SAMPLES), -64, 64)
    weights = jax.random.randint(weight_key, (STREAMS,), 0, 2)
    delay = jax.random.randint(delay_key, (), 0, 8)
    delayed = jnp.roll(common, delay, axis=1)
    antenna = (jnp.arange(STREAMS) >= 2).astype(jnp.int32)
    chosen = jnp.where(antenna[:, None, None] == 1, delayed[None], common[None])
    return (noise + weights[:, None, None] * chosen).astype(jnp.int32)


def draw_pairs(key, part):
    order = jax.random.permutation(jax.random.fold_in(key, 21), 4)
    return jnp.stack([order // 2, 2 + order % 2], axis=1).astype(jnp.int32)


def gaussian(key, dims, width, most, held_as=jnp.bfloat16):
    return jnp.clip(width * jax.random.normal(key, dims, jnp.float32), -most, most).astype(held_as)


def setup_inputs(seed: int = 0, part: int = 0) -> dict:
    seeds = jax.random.split(jax.random.key(seed), 4)
    part_keys = jax.random.split(jax.random.fold_in(seeds[3], part), 4)
    volts = draw_volts(jax.random.fold_in(jax.random.fold_in(seeds[3], part), 71), part)
    taps = gaussian(seeds[1], (TAPS, CHANNELS), 0.004, 0.024, jnp.float32)
    pairs = draw_pairs(jax.random.fold_in(seeds[3], 71), part)
    return dict(volts=volts, taps=taps, pairs=pairs)


def reference(volts, taps, pairs):
    samples = volts.astype(jnp.float32).reshape(STREAMS, 2, FRAMES, CHANNELS)
    padded = jnp.pad(samples, ((0, 0), (0, 0), (TAPS - 1, 0), (0, 0)))
    filtered = jnp.zeros((STREAMS, 2, FRAMES, CHANNELS), jnp.float32)
    for tap_index in range(TAPS):
        begin = TAPS - 1 - tap_index
        filtered = filtered + taps[tap_index] * padded[:, :, begin:begin + FRAMES]
    spectra = jnp.fft.fft(filtered[:, 0] + 1j * filtered[:, 1], axis=-1) / jnp.sqrt(jnp.float32(CHANNELS))
    real_part = jnp.real(spectra).astype(jnp.float32)
    imag_part = jnp.imag(spectra).astype(jnp.float32)
    auto = lax.optimization_barrier(jnp.sum(real_part * real_part + imag_part * imag_part, axis=1)) / FRAMES
    first = pairs[:, 0]
    second = pairs[:, 1]
    left_re = real_part[first]
    left_im = imag_part[first]
    right_re = real_part[second]
    right_im = imag_part[second]
    prod_re = left_re * right_re + left_im * right_im
    prod_im = left_im * right_re - left_re * right_im
    cross_re = lax.optimization_barrier(jnp.sum(prod_re, axis=1)) / FRAMES
    cross_im = lax.optimization_barrier(jnp.sum(prod_im, axis=1)) / FRAMES
    denom = (auto[first] + 1e-06) * (auto[second] + 1e-06)
    coherence = (cross_re * cross_re + cross_im * cross_im) / denom
    factor = 1.0 / jnp.sqrt(denom)
    normalized = jnp.stack([prod_re * factor[:, None], prod_im * factor[:, None]])
    return (coherence, normalized)
```

```python
import functools
import math

import jax
import jax.numpy as jnp
import numpy as np
from jax import lax
from jax.experimental import pallas as pl
from jax.experimental.pallas import tpu as pltpu
from jax.sharding import PartitionSpec as P

LANES = 128
SUB = 8


def matrices(channels):
    radix = channels // LANES
    lane = np.arange(LANES)
    a = (LANES // radix) * (lane % radix) + lane // radix
    angle = 2.0 * np.pi * ((a[:, None] * lane[None, :]) % LANES) / LANES
    c, s = np.cos(angle), np.sin(angle)
    full = np.block([[c, -s], [s, c]]) / math.sqrt(channels)
    high = full.astype(jnp.bfloat16)
    low = (full - high.astype(np.float64)).astype(jnp.bfloat16)
    return jnp.asarray(high), jnp.asarray(low)


def twiddles(channels):
    radix = channels // LANES
    b = np.arange(radix)
    k = np.arange(LANES)
    angle = 2.0 * np.pi * ((b[:, None] * k[None, :]) % channels) / channels
    both = np.stack([np.cos(angle), np.sin(angle)]).astype(np.float32)
    return jnp.asarray(np.broadcast_to(both[:, :, None], (2, radix, SUB, LANES)))


def turn(z, num, den):
    re, im = z
    num = num % den
    if num == 0:
        return z
    if 4 * num == den:
        return (im, -re)
    if 2 * num == den:
        return (-re, -im)
    if 4 * num == 3 * den:
        return (-im, re)
    h = np.float32(math.sqrt(0.5))
    if 8 * num == den:
        return ((re + im) * h, (im - re) * h)
    if 8 * num == 3 * den:
        return ((im - re) * h, -((re + im) * h))
    c = np.float32(math.cos(2.0 * math.pi * num / den))
    s = np.float32(math.sin(2.0 * math.pi * num / den))
    return (re * c + im * s, im * c - re * s)


def add(x, y):
    return (x[0] + y[0], x[1] + y[1])


def sub(x, y):
    return (x[0] - y[0], x[1] - y[1])


def dft(items):
    n = len(items)
    if n == 1:
        return items
    if n == 2:
        return [add(*items), sub(*items)]
    if n == 4:
        p, q = add(items[0], items[2]), sub(items[0], items[2])
        r, s = add(items[1], items[3]), sub(items[1], items[3])
        down = (q[0] + s[1], q[1] - s[0])
        up = (q[0] - s[1], q[1] + s[0])
        return [add(p, r), down, sub(p, r), up]
    if n == 8:
        even, odd = dft(items[0::2]), dft(items[1::2])
        odd = [turn(z, i, 8) for i, z in enumerate(odd)]
        return [add(e, o) for e, o in zip(even, odd)] + [sub(e, o) for e, o in zip(even, odd)]
    inner = n // 4
    groups = [[turn(z, g * i, n) for i, z in enumerate(dft(items[g::4]))] for g in range(4)]
    out = [None] * n
    for i in range(inner):
        for j, z in enumerate(dft([groups[g][i] for g in range(4)])):
            out[i + inner * j] = z
    return out


def swap_lanes(rows):
    rows = list(rows)
    lane = lax.broadcasted_iota(jnp.int32, (SUB, LANES), 1)
    step = 1
    while step < len(rows):
        low = (lane & step) == 0
        for i in range(len(rows)):
            if i & step == 0:
                a, b = rows[i], rows[i + step]
                rows[i] = jnp.where(low, a, pltpu.roll(b, step, 1))
                rows[i + step] = jnp.where(low, pltpu.roll(a, LANES - step, 1), b)
        step *= 2
    return rows


def block_work(load, pairs, taps, high, low, twist, out, acc, filt, left_hi, left_lo, mid, spec):
    streams = spec.shape[0]
    ntaps, rows_frame = taps.shape[0], taps.shape[1]
    radix = rows_frame // 2

    @pl.loop(0, streams)
    def _(s):
        @pl.loop(0, rows_frame // SUB)
        def _(c):
            rows = pl.ds(pl.multiple_of(c * SUB, SUB), SUB)
            tap = [taps[t, rows, :] for t in range(ntaps)]
            x = [load(s, i, rows).astype(jnp.float32) for i in range(SUB + ntaps - 1)]
            for f in range(SUB):
                total = tap[0] * x[f + ntaps - 1]
                for t in range(1, ntaps):
                    total = total + tap[t] * x[f + ntaps - 1 - t]
                at = pl.multiple_of(f * rows_frame + c * SUB, SUB)
                filt[s, pl.ds(at, SUB), :] = total

        for comp in range(2):
            rows = [filt[s, pl.ds(2 * r + comp, SUB, stride=rows_frame), :] for r in range(radix)]
            rows = swap_lanes(rows)
            for b in range(0, radix, 2):
                both = jnp.concatenate([rows[b], rows[b + 1]], axis=0)
                hi = both.astype(jnp.bfloat16)
                lo = (both - hi.astype(jnp.float32)).astype(jnp.bfloat16)
                at = pl.multiple_of(s * radix * SUB + b * SUB, 2 * SUB)
                where = (pl.ds(at, 2 * SUB), pl.ds(comp * LANES, LANES))
                left_hi[where] = hi
                left_lo[where] = lo

    dot = functools.partial(jnp.dot, preferred_element_type=jnp.float32)

    @pl.loop(0, streams)
    def _(s):
        at = pl.ds(pl.multiple_of(s * radix * SUB, radix * SUB), radix * SUB)
        hi, lo = left_hi[at, :], left_lo[at, :]
        mid[at, :] = dot(hi, high[...]) + (dot(lo, high[...]) + dot(hi, low[...]))

    @pl.loop(0, streams)
    def _(s):
        items = []
        for b in range(radix):
            at = pl.ds(pl.multiple_of(s * radix * SUB + b * SUB, SUB), SUB)
            re, im = mid[at, 0:LANES], mid[at, LANES : 2 * LANES]
            if b:
                c, n = twist[0, b], twist[1, b]
                re, im = re * c + im * n, im * c - re * n
            items.append((re, im))
        for k, z in enumerate(dft(items)):
            spec[s, 0, k] = z[0]
            spec[s, 1, k] = z[1]

    npairs = pairs.shape[0]

    @pl.loop(0, radix)
    def _(k):
        cols = pl.ds(pl.multiple_of(k * LANES, LANES), LANES)
        for s in range(streams):
            re, im = spec[s, 0, k], spec[s, 1, k]
            acc[s, :, cols] += re * re + im * im
        for p in range(npairs):
            a, b = pairs[p, 0], pairs[p, 1]
            lr, li, rr, ri = spec[a, 0, k], spec[a, 1, k], spec[b, 0, k], spec[b, 1, k]
            pr = lr * rr + li * ri
            pi = li * rr - lr * ri
            out[0, p, :, cols] = pr
            out[1, p, :, cols] = pi
            acc[streams + p, :, cols] += pr
            acc[streams + npairs + p, :, cols] += pi


def finish(acc, sums):
    for i in range(acc.shape[0]):
        sums[i : i + 1, :] = jnp.sum(acc[i], axis=0, keepdims=True)


def inner_kernel(pairs, pp, p, c, taps, high, low, twist, out, sums, acc, *scratch):
    j = pl.program_id(0)

    @pl.when(j == 0)
    def _():
        acc[...] = jnp.zeros_like(acc)

    def load(s, i, rows):
        if i < 7:
            return pp[s, i + 1, rows, :]
        if i < 15:
            return p[s, i - 7, rows, :]
        return c[s, i - 15, rows, :]

    block_work(load, pairs, taps, high, low, twist, out, acc, *scratch)

    @pl.when(j == pl.num_programs(0) - 1)
    def _():
        finish(acc, sums)


def edge_kernel(pairs, halo, c0, c, taps, high, low, twist, _, out, sums, acc, *scratch):
    j = pl.program_id(0)

    @pl.when(j == 0)
    def _():
        acc[...] = jnp.zeros_like(acc)

    def load(s, i, rows):
        if i < 7:
            return halo[s, i + j * SUB, rows, :]
        if i < 15:
            return jnp.where(j == 0, halo[s, i, rows, :], c0[s, i - 7, rows, :])
        return c[s, i - 15, rows, :]

    block_work(load, pairs, taps, high, low, twist, out, acc, *scratch)

    @pl.when(j == pl.num_programs(0) - 1)
    def _():
        finish(acc, sums)


def scale_kernel(frames_all, pairs, sums, prod, coherence, out):
    npairs = pairs.shape[0]
    streams = sums.shape[0] - 2 * npairs
    for p in range(npairs):
        a, b = pairs[p, 0], pairs[p, 1]
        mean_a = sums[pl.ds(a, 1), :] / frames_all
        mean_b = sums[pl.ds(b, 1), :] / frames_all
        re = sums[streams + p : streams + p + 1, :] / frames_all
        im = sums[streams + npairs + p : streams + npairs + p + 1, :] / frames_all
        denom = (mean_a + 1e-06) * (mean_b + 1e-06)

        @pl.when(pl.program_id(0) == 0)
        def _():
            coherence[p : p + 1, :] = (re * re + im * im) / denom

        factor = 1.0 / jnp.sqrt(denom)
        out[0, p] = prod[0, p] * factor
        out[1, p] = prod[1, p] * factor


def on_device(volts, taps, pairs):
    streams, comps, local = volts.shape
    ntaps, channels = taps.shape
    radix = channels // LANES
    edge = ntaps - 1
    frames = local // channels
    rows_frame = radix * comps
    blocks = frames // SUB
    npairs = pairs.shape[0]
    nsums = streams + 2 * npairs
    view = volts.reshape(streams, comps, frames * radix, LANES).transpose(0, 2, 1, 3)
    view = view.reshape(streams, frames, rows_frame, LANES)
    size = lax.axis_size("tm")
    halo = lax.ppermute(view[:, frames - edge :], "tm", [(i, i + 1) for i in range(size - 1)])
    taps2 = jnp.repeat(taps.reshape(ntaps, radix, LANES), comps, axis=1)
    high, low = matrices(channels)
    twist = twiddles(channels)

    rows = streams * radix * SUB
    scratch = [
        pltpu.VMEM((nsums, SUB, channels), jnp.float32),
        pltpu.VMEM((streams, SUB * rows_frame, LANES), jnp.float32),
        pltpu.VMEM((rows, 2 * LANES), jnp.bfloat16),
        pltpu.VMEM((rows, 2 * LANES), jnp.bfloat16),
        pltpu.VMEM((rows, 2 * LANES), jnp.float32),
        pltpu.VMEM((streams, comps, radix, SUB, LANES), jnp.float32),
    ]
    smem = pl.BlockSpec(memory_space=pltpu.SMEM)

    def whole(*dims):
        return pl.BlockSpec(dims, lambda j: (0,) * len(dims))

    tables = [
        whole(ntaps, rows_frame, LANES),
        whole(2 * LANES, 2 * LANES),
        whole(2 * LANES, 2 * LANES),
        whole(2, radix, SUB, LANES),
    ]
    frame_dims = (streams, SUB, rows_frame, LANES)
    prod_dims = (2, npairs, SUB, channels)
    prod_type = jax.ShapeDtypeStruct((2, npairs, frames, channels), jnp.float32)
    sums_type = jax.ShapeDtypeStruct((nsums, channels), jnp.float32)
    first = 2

    def params():
        return pltpu.CompilerParams(vmem_limit_bytes=48 * 1024 * 1024)

    def cost(n):
        return pl.CostEstimate(flops=n * 500_000_000, bytes_accessed=n * 4_000_000, transcendentals=0)

    prod, sums_inner = pl.pallas_call(
        inner_kernel,
        grid=(blocks - first,),
        in_specs=[smem]
        + [pl.BlockSpec(frame_dims, functools.partial(lambda d, j: (0, j + d, 0, 0), d)) for d in range(3)]
        + tables,
        out_specs=[
            pl.BlockSpec(prod_dims, lambda j: (0, 0, j + first, 0)),
            whole(nsums, channels),
        ],
        out_shape=[prod_type, sums_type],
        scratch_shapes=scratch,
        compiler_params=params(),
        cost_estimate=cost(blocks - first),
        name="inner",
    )(pairs, view, view, view, taps2, high, low, twist)

    prod, sums_edge = pl.pallas_call(
        edge_kernel,
        grid=(first,),
        in_specs=[smem, whole(streams, edge, rows_frame, LANES), whole(*frame_dims)]
        + [pl.BlockSpec(frame_dims, lambda j: (0, j, 0, 0))]
        + tables
        + [pl.BlockSpec(memory_space=pl.ANY)],
        out_specs=[
            pl.BlockSpec(prod_dims, lambda j: (0, 0, j, 0)),
            whole(nsums, channels),
        ],
        out_shape=[prod_type, sums_type],
        scratch_shapes=scratch,
        input_output_aliases={8: 0},
        compiler_params=params(),
        cost_estimate=cost(first),
        name="edge",
    )(pairs, halo, view, view, taps2, high, low, twist, prod)

    sums = lax.psum(sums_inner + sums_edge, "tm")
    coherence, normalized = pl.pallas_call(
        functools.partial(scale_kernel, frames * size),
        grid=(blocks,),
        in_specs=[smem, whole(nsums, channels), pl.BlockSpec(prod_dims, lambda j: (0, 0, j, 0))],
        out_specs=[whole(npairs, channels), pl.BlockSpec(prod_dims, lambda j: (0, 0, j, 0))],
        out_shape=[jax.ShapeDtypeStruct((npairs, channels), jnp.float32), prod_type],
        compiler_params=params(),
        name="scale",
    )(pairs, sums, prod)
    return (coherence, normalized)


def solution(mesh):
    return jax.shard_map(
        on_device,
        mesh=mesh,
        in_specs=(P("band", None, "tm"), P(), P()),
        out_specs=(P("band", None), P(None, "band", "tm", None)),
        check_vma=False,
    )
```

```python
import functools
import math

import jax
import jax.numpy as jnp
import numpy as np
from jax import lax
from jax.experimental import pallas as pl
from jax.experimental.pallas import tpu as pltpu
from jax.sharding import PartitionSpec as P

LANES = 128
SUB = 8


def matrices(channels):
    radix = channels // LANES
    lane = np.arange(LANES)
    a = (LANES // radix) * (lane % radix) + lane // radix
    angle = 2.0 * np.pi * ((a[:, None] * lane[None, :]) % LANES) / LANES
    c, s = np.cos(angle), np.sin(angle)
    full = np.block([[c, -s], [s, c]]) / math.sqrt(channels)
    high = full.astype(jnp.bfloat16)
    low = (full - high.astype(np.float64)).astype(jnp.bfloat16)
    return jnp.asarray(np.stack([high, low]))


def twiddles(channels):
    radix = channels // LANES
    b = np.arange(radix)
    k = np.arange(LANES)
    angle = 2.0 * np.pi * ((b[:, None] * k[None, :]) % channels) / channels
    both = np.stack([np.cos(angle), np.sin(angle)]).astype(np.float32)
    return jnp.asarray(both)


def turn(z, num, den):
    re, im = z
    num = num % den
    if num == 0:
        return z
    if 4 * num == den:
        return (im, -re)
    if 2 * num == den:
        return (-re, -im)
    if 4 * num == 3 * den:
        return (-im, re)
    h = np.float32(math.sqrt(0.5))
    if 8 * num == den:
        return ((re + im) * h, (im - re) * h)
    if 8 * num == 3 * den:
        return ((im - re) * h, -((re + im) * h))
    c = np.float32(math.cos(2.0 * math.pi * num / den))
    s = np.float32(math.sin(2.0 * math.pi * num / den))
    return (re * c + im * s, im * c - re * s)


def add(x, y):
    return (x[0] + y[0], x[1] + y[1])


def sub(x, y):
    return (x[0] - y[0], x[1] - y[1])


def dft(items):
    n = len(items)
    if n == 1:
        return items
    if n == 2:
        return [add(*items), sub(*items)]
    if n == 4:
        p, q = add(items[0], items[2]), sub(items[0], items[2])
        r, s = add(items[1], items[3]), sub(items[1], items[3])
        down = (q[0] + s[1], q[1] - s[0])
        up = (q[0] - s[1], q[1] + s[0])
        return [add(p, r), down, sub(p, r), up]
    if n == 8:
        even, odd = dft(items[0::2]), dft(items[1::2])
        odd = [turn(z, i, 8) for i, z in enumerate(odd)]
        return [add(e, o) for e, o in zip(even, odd)] + [sub(e, o) for e, o in zip(even, odd)]
    inner = n // 4
    groups = [[turn(z, g * i, n) for i, z in enumerate(dft(items[g::4]))] for g in range(4)]
    out = [None] * n
    for i in range(inner):
        for j, z in enumerate(dft([groups[g][i] for g in range(4)])):
            out[i + inner * j] = z
    return out


def swap_lanes(rows):
    rows = list(rows)
    lane = lax.broadcasted_iota(jnp.int32, (SUB, LANES), 1)
    step = 1
    while step < len(rows):
        low = (lane & step) == 0
        for i in range(len(rows)):
            if i & step == 0:
                a, b = rows[i], rows[i + step]
                rows[i] = jnp.where(low, a, pltpu.roll(b, step, 1))
                rows[i + step] = jnp.where(low, pltpu.roll(a, LANES - step, 1), b)
        step *= 2
    return rows


def block_work(load, pairs, taps, weights, twist, out, acc, tapd, filt, left_hi, left_lo, mid, spec):
    streams = spec.shape[0]
    ntaps, radix = taps.shape[0], taps.shape[1] // LANES
    rows_frame = 2 * radix

    @pl.when(pl.program_id(0) == 0)
    def _():
        acc[...] = jnp.zeros_like(acc)
        for r in range(radix):
            row = taps[:, r * LANES : (r + 1) * LANES]
            for comp in range(2):
                tapd[pl.ds(2 * r + comp, ntaps, stride=rows_frame), :] = row

    @pl.loop(0, streams)
    def _(s):
        @pl.loop(0, rows_frame // SUB)
        def _(c):
            rows = pl.ds(pl.multiple_of(c * SUB, SUB), SUB)
            tap = [
                tapd[pl.ds(pl.multiple_of(t * rows_frame + c * SUB, SUB), SUB), :]
                for t in range(ntaps)
            ]
            x = [load(s, i, rows).astype(jnp.float32) for i in range(SUB + ntaps - 1)]
            for f in range(SUB):
                total = tap[0] * x[f + ntaps - 1]
                for t in range(1, ntaps):
                    total = total + tap[t] * x[f + ntaps - 1 - t]
                at = pl.multiple_of(f * rows_frame + c * SUB, SUB)
                filt[s, pl.ds(at, SUB), :] = total

        for comp in range(2):
            rows = [filt[s, pl.ds(2 * r + comp, SUB, stride=rows_frame), :] for r in range(radix)]
            rows = swap_lanes(rows)
            for b in range(0, radix, 2):
                both = jnp.concatenate([rows[b], rows[b + 1]], axis=0)
                hi = both.astype(jnp.bfloat16)
                lo = (both - hi.astype(jnp.float32)).astype(jnp.bfloat16)
                at = pl.multiple_of(s * radix * SUB + b * SUB, 2 * SUB)
                where = (pl.ds(at, 2 * SUB), pl.ds(comp * LANES, LANES))
                left_hi[where] = hi
                left_lo[where] = lo

    dot = functools.partial(jnp.dot, preferred_element_type=jnp.float32)

    @pl.loop(0, streams)
    def _(s):
        at = pl.ds(pl.multiple_of(s * radix * SUB, radix * SUB), radix * SUB)
        hi, lo = left_hi[at, :], left_lo[at, :]
        mid[at, :] = dot(hi, weights[0]) + (dot(lo, weights[0]) + dot(hi, weights[1]))

    @pl.loop(0, streams)
    def _(s):
        items = []
        for b in range(radix):
            at = pl.ds(pl.multiple_of(s * radix * SUB + b * SUB, SUB), SUB)
            re, im = mid[at, 0:LANES], mid[at, LANES : 2 * LANES]
            if b:
                c, n = twist[0, b : b + 1, :], twist[1, b : b + 1, :]
                re, im = re * c + im * n, im * c - re * n
            items.append((re, im))
        for k, z in enumerate(dft(items)):
            spec[s, 0, k] = z[0]
            spec[s, 1, k] = z[1]

    npairs = pairs.shape[1]

    @pl.loop(0, radix)
    def _(k):
        cols = pl.ds(pl.multiple_of(k * LANES, LANES), LANES)
        for s in range(streams):
            re, im = spec[s, 0, k], spec[s, 1, k]
            acc[s, :, cols] += re * re + im * im
        for p in range(npairs):
            a, b = pairs[0, p], pairs[1, p]
            lr, li, rr, ri = spec[a, 0, k], spec[a, 1, k], spec[b, 0, k], spec[b, 1, k]
            pr = lr * rr + li * ri
            pi = li * rr - lr * ri
            out[0, p, :, cols] = pr
            out[1, p, :, cols] = pi
            acc[streams + p, :, cols] += pr
            acc[streams + npairs + p, :, cols] += pi


def finish(acc, sums):
    for i in range(acc.shape[0]):
        sums[i : i + 1, :] = jnp.sum(acc[i], axis=0, keepdims=True)


def inner_kernel(pairs, pp, p, c, taps, weights, twist, out, sums, acc, *scratch):
    j = pl.program_id(0)

    def load(s, i, rows):
        if i < 7:
            return pp[s, i + 1, rows, :]
        if i < 15:
            return p[s, i - 7, rows, :]
        return c[s, i - 15, rows, :]

    block_work(load, pairs, taps, weights, twist, out, acc, *scratch)

    @pl.when(j == pl.num_programs(0) - 1)
    def _():
        finish(acc, sums)


def edge_kernel(pairs, halo, c0, c, taps, weights, twist, _, out, sums, acc, *scratch):
    j = pl.program_id(0)

    def load(s, i, rows):
        if i < 7:
            return halo[s, i + j * SUB, rows, :]
        if i < 15:
            return jnp.where(j == 0, halo[s, i, rows, :], c0[s, i - 7, rows, :])
        return c[s, i - 15, rows, :]

    block_work(load, pairs, taps, weights, twist, out, acc, *scratch)

    @pl.when(j == pl.num_programs(0) - 1)
    def _():
        finish(acc, sums)


def reduce_kernel(n, owners, frames_all, pairs, a, b, out, send, recv, part, got, s1, r1, s2, r2):
    me = lax.axis_index("tm")
    radix = send.shape[0]
    per = radix // owners
    npairs = pairs.shape[1]
    streams = send.shape[1] - 2 * npairs
    everyone = owners == n

    def peer(d):
        return lax.rem(me + d, n)

    def source(d):
        return lax.rem(me + n - d, n)

    def guarded(cond, do):
        if everyone:
            do()
        else:
            pl.when(cond)(do)

    def scatter(d):
        return pltpu.make_async_remote_copy(
            src_ref=send.at[pl.ds(peer(d) * per, per)],
            dst_ref=recv.at[d],
            send_sem=s1.at[d],
            recv_sem=r1.at[d],
            device_id={"tm": peer(d)},
            device_id_type=pl.DeviceIdType.MESH,
        )

    def spread(d, owner):
        return pltpu.make_async_remote_copy(
            src_ref=part,
            dst_ref=got.at[pl.ds(owner * per, per)],
            send_sem=s2.at[d],
            recv_sem=r2.at[d],
            device_id={"tm": peer(d)},
            device_id_type=pl.DeviceIdType.MESH,
        )

    barrier = pltpu.get_barrier_semaphore()

    @pl.loop(1, n)
    def _(d):
        pl.semaphore_signal(
            barrier, inc=1, device_id={"tm": peer(d)}, device_id_type=pl.DeviceIdType.MESH
        )

    for k in range(radix):
        cols = slice(k * LANES, (k + 1) * LANES)
        send[k] = a[:, cols] + b[:, cols]
    pl.semaphore_wait(barrier, n - 1)

    @pl.loop(1, n)
    def _(d):
        guarded(peer(d) < owners, lambda: scatter(d).start())

    def own():
        @pl.loop(1, n)
        def _(d):
            scatter(d).wait_recv()

        def more(d, total):
            return total + recv[d]

        total = lax.fori_loop(1, n, more, send[pl.ds(me * per, per)]) / frames_all
        auto = [total[:, s : s + 1, :] + 1e-06 for s in range(streams)]

        def pick(s):
            value = auto[0]
            for i in range(1, streams):
                value = jnp.where(s == i, auto[i], value)
            return value

        for p in range(npairs):
            re = total[:, streams + p : streams + p + 1, :]
            im = total[:, streams + npairs + p : streams + npairs + p + 1, :]
            denom = pick(pairs[0, p]) * pick(pairs[1, p])
            part[:, p : p + 1, :] = 1.0 / jnp.sqrt(denom)
            part[:, npairs + p : npairs + p + 1, :] = (re * re + im * im) / denom

        @pl.loop(1, n)
        def _(d):
            spread(d, me).start()

        got[pl.ds(me * per, per)] = part[...]

    guarded(me < owners, own)

    @pl.loop(1, n)
    def _(d):
        guarded(source(d) < owners, lambda: spread(d, source(d)).wait_recv())

    out[...] = got[...]

    @pl.loop(1, n)
    def _(d):
        guarded(peer(d) < owners, lambda: scatter(d).wait_send())
        guarded(me < owners, lambda: spread(d, me).wait_send())


def scale_kernel(table, prod, coherence, out):
    npairs = prod.shape[1]

    @pl.when(pl.program_id(0) == 0)
    def _():
        for k in range(table.shape[0]):
            coherence[:, k * LANES : (k + 1) * LANES] = table[k, npairs:, :]

    for k in range(table.shape[0]):
        cols = slice(k * LANES, (k + 1) * LANES)
        for p in range(npairs):
            factor = table[k, p : p + 1, :]
            out[0, p, :, cols] = prod[0, p, :, cols] * factor
            out[1, p, :, cols] = prod[1, p, :, cols] * factor


def on_device(volts, taps, pairs):
    streams, comps, local = volts.shape
    ntaps, channels = taps.shape
    radix = channels // LANES
    edge = ntaps - 1
    frames = local // channels
    rows_frame = radix * comps
    blocks = frames // SUB
    npairs = pairs.shape[0]
    nsums = streams + 2 * npairs
    view = volts.reshape(streams, comps, frames * radix, LANES).transpose(0, 2, 1, 3)
    view = view.reshape(streams, frames, rows_frame, LANES)
    size = lax.axis_size("tm")
    halo = lax.ppermute(view[:, frames - edge :], "tm", [(i, i + 1) for i in range(size - 1)])
    pairs = pairs.T
    weights = matrices(channels)
    twist = twiddles(channels)

    rows = streams * radix * SUB
    scratch = [
        pltpu.VMEM((nsums, SUB, channels), jnp.float32),
        pltpu.VMEM((ntaps * rows_frame, LANES), jnp.float32),
        pltpu.VMEM((streams, SUB * rows_frame, LANES), jnp.float32),
        pltpu.VMEM((rows, 2 * LANES), jnp.bfloat16),
        pltpu.VMEM((rows, 2 * LANES), jnp.bfloat16),
        pltpu.VMEM((rows, 2 * LANES), jnp.float32),
        pltpu.VMEM((streams, comps, radix, SUB, LANES), jnp.float32),
    ]
    smem = pl.BlockSpec(memory_space=pltpu.SMEM)

    def whole(*dims):
        return pl.BlockSpec(dims, lambda j: (0,) * len(dims))

    tables = [
        whole(ntaps, channels),
        whole(2, 2 * LANES, 2 * LANES),
        whole(2, radix, LANES),
    ]
    frame_dims = (streams, SUB, rows_frame, LANES)
    prod_dims = (2, npairs, SUB, channels)
    prod_type = jax.ShapeDtypeStruct((2, npairs, frames, channels), jnp.float32)
    sums_type = jax.ShapeDtypeStruct((nsums, channels), jnp.float32)
    first = 2

    def params():
        return pltpu.CompilerParams(vmem_limit_bytes=48 * 1024 * 1024)

    def cost(n):
        return pl.CostEstimate(flops=n * 500_000_000, bytes_accessed=n * 4_000_000, transcendentals=0)

    prod, sums_inner = pl.pallas_call(
        inner_kernel,
        grid=(blocks - first,),
        in_specs=[smem]
        + [pl.BlockSpec(frame_dims, functools.partial(lambda d, j: (0, j + d, 0, 0), d)) for d in range(3)]
        + tables,
        out_specs=[
            pl.BlockSpec(prod_dims, lambda j: (0, 0, j + first, 0)),
            whole(nsums, channels),
        ],
        out_shape=[prod_type, sums_type],
        scratch_shapes=scratch,
        compiler_params=params(),
        cost_estimate=cost(blocks - first),
        name="inner",
    )(pairs, view, view, view, taps, weights, twist)

    prod, sums_edge = pl.pallas_call(
        edge_kernel,
        grid=(first,),
        in_specs=[smem, whole(streams, edge, rows_frame, LANES), whole(*frame_dims)]
        + [pl.BlockSpec(frame_dims, lambda j: (0, j, 0, 0))]
        + tables
        + [pl.BlockSpec(memory_space=pl.ANY)],
        out_specs=[
            pl.BlockSpec(prod_dims, lambda j: (0, 0, j, 0)),
            whole(nsums, channels),
        ],
        out_shape=[prod_type, sums_type],
        scratch_shapes=scratch,
        input_output_aliases={7: 0},
        compiler_params=params(),
        cost_estimate=cost(first),
        name="edge",
    )(pairs, halo, view, view, taps, weights, twist, prod)

    owners = math.gcd(size, radix)
    per = radix // owners
    vmem = pl.BlockSpec(memory_space=pltpu.VMEM)
    dma = pltpu.SemaphoreType.DMA((size,))
    table = pl.pallas_call(
        functools.partial(reduce_kernel, size, owners, frames * size),
        in_specs=[smem, vmem, vmem],
        out_specs=vmem,
        out_shape=jax.ShapeDtypeStruct((radix, 2 * npairs, LANES), jnp.float32),
        scratch_shapes=[
            pltpu.VMEM((radix, nsums, LANES), jnp.float32),
            pltpu.VMEM((size, per, nsums, LANES), jnp.float32),
            pltpu.VMEM((per, 2 * npairs, LANES), jnp.float32),
            pltpu.VMEM((radix, 2 * npairs, LANES), jnp.float32),
            dma,
            dma,
            dma,
            dma,
        ],
        compiler_params=pltpu.CompilerParams(collective_id=0, has_side_effects=True),
        name="reduce",
    )(pairs, sums_inner, sums_edge)

    coherence, normalized = pl.pallas_call(
        scale_kernel,
        grid=(blocks,),
        in_specs=[
            whole(radix, 2 * npairs, LANES),
            pl.BlockSpec(prod_dims, lambda j: (0, 0, j, 0)),
        ],
        out_specs=[whole(npairs, channels), pl.BlockSpec(prod_dims, lambda j: (0, 0, j, 0))],
        out_shape=[jax.ShapeDtypeStruct((npairs, channels), jnp.float32), prod_type],
        compiler_params=params(),
        name="scale",
    )(table, prod)
    return (coherence, normalized)


def solution(mesh):
    return jax.shard_map(
        on_device,
        mesh=mesh,
        in_specs=(P("band", None, "tm"), P(), P()),
        out_specs=(P("band", None), P(None, "band", "tm", None)),
        check_vma=False,
    )
```

```python
import functools
import math

import jax
import jax.numpy as jnp
import numpy as np
from jax import lax
from jax.experimental import pallas as pl
from jax.experimental.pallas import tpu as pltpu
from jax.sharding import PartitionSpec as P

LANES = 128
SUB = 8


def matrices(channels):
    radix = channels // LANES
    lane = np.arange(LANES)
    a = (LANES // radix) * (lane % radix) + lane // radix
    angle = 2.0 * np.pi * ((a[:, None] * lane[None, :]) % LANES) / LANES
    c, s = np.cos(angle), np.sin(angle)
    full = np.block([[c, -s], [s, c]]) / math.sqrt(channels)
    high = full.astype(jnp.bfloat16)
    low = (full - high.astype(np.float64)).astype(jnp.bfloat16)
    return jnp.asarray(np.stack([high, low]))


def twiddles(channels):
    radix = channels // LANES
    b = np.arange(radix)
    k = np.arange(LANES)
    angle = 2.0 * np.pi * ((b[:, None] * k[None, :]) % channels) / channels
    both = np.stack([np.cos(angle), np.sin(angle)]).astype(np.float32)
    return jnp.asarray(both)


def turn(z, num, den):
    re, im = z
    num = num % den
    if num == 0:
        return z
    if 4 * num == den:
        return (im, -re)
    if 2 * num == den:
        return (-re, -im)
    if 4 * num == 3 * den:
        return (-im, re)
    h = np.float32(math.sqrt(0.5))
    if 8 * num == den:
        return ((re + im) * h, (im - re) * h)
    if 8 * num == 3 * den:
        return ((im - re) * h, -((re + im) * h))
    c = np.float32(math.cos(2.0 * math.pi * num / den))
    s = np.float32(math.sin(2.0 * math.pi * num / den))
    return (re * c + im * s, im * c - re * s)


def add(x, y):
    return (x[0] + y[0], x[1] + y[1])


def sub(x, y):
    return (x[0] - y[0], x[1] - y[1])


def dft(items):
    n = len(items)
    if n == 1:
        return items
    if n == 2:
        return [add(*items), sub(*items)]
    if n == 4:
        p, q = add(items[0], items[2]), sub(items[0], items[2])
        r, s = add(items[1], items[3]), sub(items[1], items[3])
        down = (q[0] + s[1], q[1] - s[0])
        up = (q[0] - s[1], q[1] + s[0])
        return [add(p, r), down, sub(p, r), up]
    if n == 8:
        even, odd = dft(items[0::2]), dft(items[1::2])
        odd = [turn(z, i, 8) for i, z in enumerate(odd)]
        return [add(e, o) for e, o in zip(even, odd)] + [sub(e, o) for e, o in zip(even, odd)]
    inner = n // 4
    groups = [[turn(z, g * i, n) for i, z in enumerate(dft(items[g::4]))] for g in range(4)]
    out = [None] * n
    for i in range(inner):
        for j, z in enumerate(dft([groups[g][i] for g in range(4)])):
            out[i + inner * j] = z
    return out


def block_work(load, pairs, taps, weights, twist, out, acc, tapd, filt, left_hi, left_lo, mid, spec):
    streams = spec.shape[0]
    ntaps, radix = taps.shape[0], taps.shape[1] // LANES
    rows_frame = 2 * radix
    pitch = rows_frame + 1

    @pl.when(pl.program_id(0) == 0)
    def _():
        acc[...] = jnp.zeros_like(acc)
        for r in range(radix):
            row = taps[:, r * LANES : (r + 1) * LANES]
            for comp in range(2):
                tapd[pl.ds(2 * r + comp, ntaps, stride=pitch), :] = row

    def fir(s, c):
        rows = pl.ds(pl.multiple_of(c * SUB, SUB), SUB)
        tap = [
            tapd[pl.ds(t * pitch + c * SUB, SUB), :]
            for t in range(ntaps)
        ]
        x = [load(s, i, rows).astype(jnp.float32) for i in range(SUB + ntaps - 1)]
        for f in range(SUB):
            total = tap[0] * x[f + ntaps - 1]
            for t in range(1, ntaps):
                total = total + tap[t] * x[f + ntaps - 1 - t]
            filt[s, pl.ds(f * pitch + c * SUB, SUB), :] = total

    def low_bit(step):
        return (lax.broadcasted_iota(jnp.int32, (SUB, LANES), 1) & step) == 0

    def exchange(a, b, step):
        low = low_bit(step)
        return (
            jnp.where(low, a, pltpu.roll(b, step, 1)),
            jnp.where(low, pltpu.roll(a, LANES - step, 1), b),
        )

    def swap(stream):
        sets = [(stream, comp) for comp in range(2)]
        for s, comp in sets:
            for g in range(0, radix, 4):
                v = [
                    filt[s, pl.ds(2 * r + comp, SUB, stride=pitch), :]
                    for r in range(g, g + 4)
                ]
                v[0], v[1] = exchange(v[0], v[1], 1)
                v[2], v[3] = exchange(v[2], v[3], 1)
                v[0], v[2] = exchange(v[0], v[2], 2)
                v[1], v[3] = exchange(v[1], v[3], 2)
                for i in range(4):
                    spec[s, comp, g + i] = v[i]
        for s, comp in sets:
            for g in [16 * h + i for h in range(radix // 16) for i in range(4)]:
                v = [spec[s, comp, g + 4 * i] for i in range(4)]
                v[0], v[1] = exchange(v[0], v[1], 4)
                v[2], v[3] = exchange(v[2], v[3], 4)
                v[0], v[2] = exchange(v[0], v[2], 8)
                v[1], v[3] = exchange(v[1], v[3], 8)
                for i in range(4):
                    spec[s, comp, g + 4 * i] = v[i]
        for s, comp in sets:
            for b in range(0, radix // 2, 2):
                v = [exchange(spec[s, comp, b + i], spec[s, comp, b + i + 16], 16) for i in range(2)]
                for half in range(2):
                    both = jnp.concatenate([v[0][half], v[1][half]], axis=0)
                    hi = both.astype(jnp.bfloat16)
                    lo = (both - hi.astype(jnp.float32)).astype(jnp.bfloat16)
                    at = pl.multiple_of(s * radix * SUB + (b + 16 * half) * SUB, 2 * SUB)
                    where = (pl.ds(at, 2 * SUB), pl.ds(comp * LANES, LANES))
                    left_hi[where] = hi
                    left_lo[where] = lo

    @pl.loop(0, rows_frame // SUB)
    def _(c):
        fir(0, c)

    @pl.loop(0, streams - 1)
    def _(s):
        swap(s)
        for c in range(rows_frame // SUB):
            fir(s + 1, c)

    swap(streams - 1)

    dot = functools.partial(jnp.dot, preferred_element_type=jnp.float32)

    @pl.loop(0, streams)
    def _(s):
        at = pl.ds(pl.multiple_of(s * radix * SUB, radix * SUB), radix * SUB)
        hi, lo = left_hi[at, :], left_lo[at, :]
        mid[at, :] = dot(hi, weights[0]) + (dot(lo, weights[0]) + dot(hi, weights[1]))

    @pl.loop(0, streams)
    def _(s):
        items = []
        for b in range(radix):
            at = pl.ds(pl.multiple_of(s * radix * SUB + b * SUB, SUB), SUB)
            re, im = mid[at, 0:LANES], mid[at, LANES : 2 * LANES]
            if b:
                c, n = twist[0, b : b + 1, :], twist[1, b : b + 1, :]
                re, im = re * c + im * n, im * c - re * n
            items.append((re, im))
        for k, z in enumerate(dft(items)):
            spec[s, 0, k] = z[0]
            spec[s, 1, k] = z[1]

    npairs = pairs.shape[1]

    @pl.loop(0, radix)
    def _(k):
        cols = pl.ds(pl.multiple_of(k * LANES, LANES), LANES)
        for s in range(streams):
            re, im = spec[s, 0, k], spec[s, 1, k]
            acc[s, :, cols] += re * re + im * im
        for p in range(npairs):
            a, b = pairs[0, p], pairs[1, p]
            lr, li, rr, ri = spec[a, 0, k], spec[a, 1, k], spec[b, 0, k], spec[b, 1, k]
            pr = lr * rr + li * ri
            pi = li * rr - lr * ri
            out[0, p, :, cols] = pr
            out[1, p, :, cols] = pi
            acc[streams + p, :, cols] += pr
            acc[streams + npairs + p, :, cols] += pi


def finish(acc, sums):
    for i in range(acc.shape[0]):
        sums[i : i + 1, :] = jnp.sum(acc[i], axis=0, keepdims=True)


def inner_kernel(pairs, pp, p, c, taps, weights, twist, out, sums, acc, *scratch):
    j = pl.program_id(0)

    def load(s, i, rows):
        if i < 7:
            return pp[s, i + 1, rows, :]
        if i < 15:
            return p[s, i - 7, rows, :]
        return c[s, i - 15, rows, :]

    block_work(load, pairs, taps, weights, twist, out, acc, *scratch)

    @pl.when(j == pl.num_programs(0) - 1)
    def _():
        finish(acc, sums)


def edge_kernel(pairs, halo, c0, c, taps, weights, twist, _, out, sums, acc, *scratch):
    j = pl.program_id(0)

    def load(s, i, rows):
        if i < 7:
            return halo[s, i + j * SUB, rows, :]
        if i < 15:
            return jnp.where(j == 0, halo[s, i, rows, :], c0[s, i - 7, rows, :])
        return c[s, i - 15, rows, :]

    block_work(load, pairs, taps, weights, twist, out, acc, *scratch)

    @pl.when(j == pl.num_programs(0) - 1)
    def _():
        finish(acc, sums)


def reduce_kernel(n, owners, frames_all, pairs, a, b, out, send, recv, part, got, s1, r1, s2, r2):
    me = lax.axis_index("tm")
    radix = send.shape[0]
    per = radix // owners
    npairs = pairs.shape[1]
    streams = send.shape[1] - 2 * npairs
    everyone = owners == n

    def peer(d):
        return lax.rem(me + d, n)

    def source(d):
        return lax.rem(me + n - d, n)

    def guarded(cond, do):
        if everyone:
            do()
        else:
            pl.when(cond)(do)

    def scatter(d):
        return pltpu.make_async_remote_copy(
            src_ref=send.at[pl.ds(peer(d) * per, per)],
            dst_ref=recv.at[d],
            send_sem=s1.at[d],
            recv_sem=r1.at[d],
            device_id={"tm": peer(d)},
            device_id_type=pl.DeviceIdType.MESH,
        )

    def spread(d, owner):
        return pltpu.make_async_remote_copy(
            src_ref=part,
            dst_ref=got.at[pl.ds(owner * per, per)],
            send_sem=s2.at[d],
            recv_sem=r2.at[d],
            device_id={"tm": peer(d)},
            device_id_type=pl.DeviceIdType.MESH,
        )

    barrier = pltpu.get_barrier_semaphore()

    @pl.loop(1, n)
    def _(d):
        pl.semaphore_signal(
            barrier, inc=1, device_id={"tm": peer(d)}, device_id_type=pl.DeviceIdType.MESH
        )

    for k in range(radix):
        cols = slice(k * LANES, (k + 1) * LANES)
        send[k] = a[:, cols] + b[:, cols]
    pl.semaphore_wait(barrier, n - 1)

    @pl.loop(1, n)
    def _(d):
        guarded(peer(d) < owners, lambda: scatter(d).start())

    def own():
        @pl.loop(1, n)
        def _(d):
            scatter(d).wait_recv()

        def more(d, total):
            return total + recv[d]

        total = lax.fori_loop(1, n, more, send[pl.ds(me * per, per)]) / frames_all
        auto = [total[:, s : s + 1, :] + 1e-06 for s in range(streams)]

        def pick(s):
            value = auto[0]
            for i in range(1, streams):
                value = jnp.where(s == i, auto[i], value)
            return value

        for p in range(npairs):
            re = total[:, streams + p : streams + p + 1, :]
            im = total[:, streams + npairs + p : streams + npairs + p + 1, :]
            denom = pick(pairs[0, p]) * pick(pairs[1, p])
            part[:, p : p + 1, :] = 1.0 / jnp.sqrt(denom)
            part[:, npairs + p : npairs + p + 1, :] = (re * re + im * im) / denom

        @pl.loop(1, n)
        def _(d):
            spread(d, me).start()

        got[pl.ds(me * per, per)] = part[...]

    guarded(me < owners, own)

    @pl.loop(1, n)
    def _(d):
        guarded(source(d) < owners, lambda: spread(d, source(d)).wait_recv())

    out[...] = got[...]

    @pl.loop(1, n)
    def _(d):
        guarded(peer(d) < owners, lambda: scatter(d).wait_send())
        guarded(me < owners, lambda: spread(d, me).wait_send())


def scale_kernel(table, prod, coherence, out):
    npairs = prod.shape[1]

    @pl.when(pl.program_id(0) == 0)
    def _():
        for k in range(table.shape[0]):
            coherence[:, k * LANES : (k + 1) * LANES] = table[k, npairs:, :]

    for k in range(table.shape[0]):
        cols = slice(k * LANES, (k + 1) * LANES)
        for p in range(npairs):
            factor = table[k, p : p + 1, :]
            out[0, p, :, cols] = prod[0, p, :, cols] * factor
            out[1, p, :, cols] = prod[1, p, :, cols] * factor


def on_device(volts, taps, pairs):
    streams, comps, local = volts.shape
    ntaps, channels = taps.shape
    radix = channels // LANES
    edge = ntaps - 1
    frames = local // channels
    rows_frame = radix * comps
    blocks = frames // SUB
    npairs = pairs.shape[0]
    nsums = streams + 2 * npairs
    view = volts.reshape(streams, comps, frames * radix, LANES).transpose(0, 2, 1, 3)
    view = view.reshape(streams, frames, rows_frame, LANES)
    size = lax.axis_size("tm")
    halo = lax.ppermute(view[:, frames - edge :], "tm", [(i, i + 1) for i in range(size - 1)])
    pairs = pairs.T
    weights = matrices(channels)
    twist = twiddles(channels)

    rows = streams * radix * SUB
    scratch = [
        pltpu.VMEM((nsums, SUB, channels), jnp.float32),
        pltpu.VMEM((ntaps * (rows_frame + 1), LANES), jnp.float32),
        pltpu.VMEM((streams, SUB * (rows_frame + 1), LANES), jnp.float32),
        pltpu.VMEM((rows, 2 * LANES), jnp.bfloat16),
        pltpu.VMEM((rows, 2 * LANES), jnp.bfloat16),
        pltpu.VMEM((rows, 2 * LANES), jnp.float32),
        pltpu.VMEM((streams, comps, radix, SUB, LANES), jnp.float32),
    ]
    smem = pl.BlockSpec(memory_space=pltpu.SMEM)

    def whole(*dims):
        return pl.BlockSpec(dims, lambda j: (0,) * len(dims))

    tables = [
        whole(ntaps, channels),
        whole(2, 2 * LANES, 2 * LANES),
        whole(2, radix, LANES),
    ]
    frame_dims = (streams, SUB, rows_frame, LANES)
    prod_dims = (2, npairs, SUB, channels)
    prod_type = jax.ShapeDtypeStruct((2, npairs, frames, channels), jnp.float32)
    sums_type = jax.ShapeDtypeStruct((nsums, channels), jnp.float32)
    first = 2

    def params():
        return pltpu.CompilerParams(vmem_limit_bytes=63 * 1024 * 1024)

    def cost(n):
        return pl.CostEstimate(flops=n * 500_000_000, bytes_accessed=n * 4_000_000, transcendentals=0)

    prod, sums_inner = pl.pallas_call(
        inner_kernel,
        grid=(blocks - first,),
        in_specs=[smem]
        + [pl.BlockSpec(frame_dims, functools.partial(lambda d, j: (0, j + d, 0, 0), d)) for d in range(3)]
        + tables,
        out_specs=[
            pl.BlockSpec(prod_dims, lambda j: (0, 0, j + first, 0)),
            whole(nsums, channels),
        ],
        out_shape=[prod_type, sums_type],
        scratch_shapes=scratch,
        compiler_params=params(),
        cost_estimate=cost(blocks - first),
        name="inner",
    )(pairs, view, view, view, taps, weights, twist)

    prod, sums_edge = pl.pallas_call(
        edge_kernel,
        grid=(first,),
        in_specs=[smem, whole(streams, edge, rows_frame, LANES), whole(*frame_dims)]
        + [pl.BlockSpec(frame_dims, lambda j: (0, j, 0, 0))]
        + tables
        + [pl.BlockSpec(memory_space=pl.ANY)],
        out_specs=[
            pl.BlockSpec(prod_dims, lambda j: (0, 0, j, 0)),
            whole(nsums, channels),
        ],
        out_shape=[prod_type, sums_type],
        scratch_shapes=scratch,
        input_output_aliases={7: 0},
        compiler_params=params(),
        cost_estimate=cost(first),
        name="edge",
    )(pairs, halo, view, view, taps, weights, twist, prod)

    owners = math.gcd(size, radix)
    per = radix // owners
    vmem = pl.BlockSpec(memory_space=pltpu.VMEM)
    dma = pltpu.SemaphoreType.DMA((size,))
    table = pl.pallas_call(
        functools.partial(reduce_kernel, size, owners, frames * size),
        in_specs=[smem, vmem, vmem],
        out_specs=vmem,
        out_shape=jax.ShapeDtypeStruct((radix, 2 * npairs, LANES), jnp.float32),
        scratch_shapes=[
            pltpu.VMEM((radix, nsums, LANES), jnp.float32),
            pltpu.VMEM((size, per, nsums, LANES), jnp.float32),
            pltpu.VMEM((per, 2 * npairs, LANES), jnp.float32),
            pltpu.VMEM((radix, 2 * npairs, LANES), jnp.float32),
            dma,
            dma,
            dma,
            dma,
        ],
        compiler_params=pltpu.CompilerParams(collective_id=0, has_side_effects=True),
        name="reduce",
    )(pairs, sums_inner, sums_edge)

    coherence, normalized = pl.pallas_call(
        scale_kernel,
        grid=(blocks,),
        in_specs=[
            whole(radix, 2 * npairs, LANES),
            pl.BlockSpec(prod_dims, lambda j: (0, 0, j, 0)),
        ],
        out_specs=[whole(npairs, channels), pl.BlockSpec(prod_dims, lambda j: (0, 0, j, 0))],
        out_shape=[jax.ShapeDtypeStruct((npairs, channels), jnp.float32), prod_type],
        compiler_params=params(),
        name="scale",
    )(table, prod)
    return (coherence, normalized)


def solution(mesh):
    return jax.shard_map(
        on_device,
        mesh=mesh,
        in_specs=(P("band", None, "tm"), P(), P()),
        out_specs=(P("band", None), P(None, "band", "tm", None)),
        check_vma=False,
    )
```
